32 devices in a mesh: gx: 4 (over x, core), gy: 8 (over z, y).
Axes of the slice: x: 2, y: 2, z: 4, core: 2. Of those that a mesh axis runs over, the one named last changes fastest.
Arguments:
- slot_tiles: int32 [32, 32], P(('gx', 'gy')), may hold values from -1 to 63, as said below
- owner_map: int32 [32], replicated, may hold values from 0 to 31, each once
- slot_depth: int32 [32, 32, 16, 128], P(('gx', 'gy')), may hold values from 0 to 1073741823
- slot_color: bfloat16 [32, 32, 16, 3, 128], P(('gx', 'gy')), may hold values from 0 to 1
Outputs:
- region_depth: int32 [32, 2, 16, 128], P(('gx', 'gy'))
- region_color: bfloat16 [32, 2, 16, 3, 128], P(('gx', 'gy'))
- thumbnail: float32 [32, 3, 64], replicated
The draws below stay inside these ranges and needn't reach their ends.
Inputs may be any that keep to these rules, and one draw needn't show every extreme that they name: `slot_tiles`: each rank's used slots name the tiles of one rectangle of at least 4 tile rows of the 8 x 8 tile grid, each once, in row-major order, followed by -1 in the unused slots; all ranks' rectangles contain a common region. `owner_map`: each rank owns exactly one region.
All inputs are finite; a program needn't handle non-finite values.
Results may differ from the reference program's by a relative error of at most 0.001.
Values may be sent and summed in bfloat16 or wider, within the bound.
A program may use at most 64 MiB of HBM per device.

```python
import jax
import jax.numpy as jnp
from jax import lax

TILE = 128
BAND = 16
TROWS = 8
TCOLS = 8
TILES = 64
SLOTS = 32
REGIONS = 32
THUMB = 64
DEVICES = 32


def box_tiles(key):
    keys = jax.random.split(jax.random.fold_in(key, 11), 9)
    focus_pair = jax.random.randint(keys[0], (), 0, TROWS // 2)
    focus_col = jax.random.randint(keys[1], (), 0, TCOLS)
    lowest = max(3, TROWS // 2)
    box_height = lowest + jax.random.randint(keys[2], (DEVICES,), 0, 1 << 20) % (TROWS - lowest + 1)
    widest = jnp.minimum(SLOTS // box_height, TCOLS)
    narrowing = jax.random.randint(keys[8], (DEVICES,), 0, 2)
    box_width = jnp.maximum(1, widest - narrowing)
    row_low = jnp.maximum(0, 2 * focus_pair + 2 - box_height)
    row_high = jnp.minimum(2 * focus_pair, TROWS - box_height)
    row_span = row_high - row_low + 1
    first_draw = jax.random.randint(keys[4], (DEVICES,), 0, 1 << 20) % row_span
    second_draw = jax.random.randint(keys[5], (DEVICES,), 0, 1 << 20) % row_span
    top_row = row_low + (first_draw + second_draw) // 2
    col_low = jnp.maximum(0, focus_col - box_width + 1)
    col_high = jnp.minimum(focus_col, TCOLS - box_width)
    col_span = col_high - col_low + 1
    third_draw = jax.random.randint(keys[6], (DEVICES,), 0, 1 << 20) % col_span
    fourth_draw = jax.random.randint(keys[7], (DEVICES,), 0, 1 << 20) % col_span
    left_col = col_low + (third_draw + fourth_draw) // 2
    slot_index = jnp.arange(SLOTS, dtype=jnp.int32)[None, :]
    inner_row = slot_index // box_width[:, None]
    inner_col = slot_index % box_width[:, None]
    is_live = slot_index < (box_height * box_width)[:, None]
    tile_ids = (top_row[:, None] + inner_row) * TCOLS + left_col[:, None] + inner_col
    return jnp.where(is_live, tile_ids, -1).astype(jnp.int32)


def draw_slot_tiles(key, part):
    return box_tiles(key)


def draw_slot_depth(key, part):
    tile_ids = box_tiles(key)
    keys = jax.random.split(jax.random.fold_in(key, 23), 3)
    surface = jax.random.randint(keys[0], (TILES, BAND, TILE), 0, 1073741823).astype(jnp.int32)
    safe_tile = jnp.where(tile_ids >= 0, tile_ids, 0).astype(jnp.int32)
    front = surface[safe_tile]
    coin = jax.random.randint(keys[1], (DEVICES, SLOTS, BAND, TILE), 0, 8)
    room = (1073741823 - front).astype(jnp.int32)
    raw_extra = jax.random.randint(keys[2], (DEVICES, SLOTS, BAND, TILE), 0, 1 << 30).astype(jnp.int32)
    extra = 1 + raw_extra % room
    return (front + jnp.where(coin == 0, 0, extra)).astype(jnp.int32)


def block_levels(own_key, extent, shards, least, top_value):
    factor_of, own = 1.0, jax.random.fold_in(own_key, 6)
    for position, parts in shards:
        steps = jnp.exp(jax.random.uniform(jax.random.fold_in(own, position), (parts,), jnp.float32, least / len(shards), top_value / len(shards)))
        factor_of = factor_of * jnp.repeat(steps, extent[position] // parts).reshape([-1 if axis == position else 1 for axis in range(len(extent))])
    return factor_of


def setup_inputs(seed: int = 0) -> dict:
    seeds = jax.random.split(jax.random.key(seed), 5)
    return {
        "slot_tiles": draw_slot_tiles(jax.random.fold_in(seeds[4], 71), 0),
        "owner_map": jax.random.permutation(seeds[1], REGIONS).astype(jnp.int32),
        "slot_depth": draw_slot_depth(jax.random.fold_in(seeds[4], 71), 0),
        "slot_color": jnp.clip(1.0 * jax.random.uniform(seeds[3], (DEVICES, SLOTS, BAND, 3, TILE), jnp.float32) ** block_levels(seeds[3], (DEVICES, SLOTS, BAND, 3, TILE), ((0, 32),), -0.2, 0.2), 0.0, 1.0).astype(jnp.bfloat16),
    }


far_depth = 1073741824


def reference(slot_tiles, owner_map, slot_depth, slot_color):
    tile_count = TROWS * TCOLS

    def place_rank(frame_state, rank_data):
        frame_depth, frame_color = frame_state
        rank_tiles, rank_depth, rank_color = rank_data
        gather_index = jnp.where(rank_tiles >= 0, rank_tiles, tile_count).astype(jnp.int32)
        current = frame_depth[gather_index]
        nearer = rank_depth < current
        new_depth = jnp.where(nearer, rank_depth, current)
        new_color = jnp.where(nearer[:, :, None, :], rank_color, frame_color[gather_index])
        return (frame_depth.at[gather_index].set(new_depth), frame_color.at[gather_index].set(new_color)), None

    start_depth = jnp.full((tile_count + 1, BAND, TILE), far_depth, jnp.int32)
    start_color = jnp.zeros((tile_count + 1, BAND, 3, TILE), jnp.bfloat16)
    final_state, unused = lax.scan(place_rank, (start_depth, start_color), (slot_tiles, slot_depth, slot_color))
    frame_depth = final_state[0][:tile_count]
    frame_color = final_state[1][:tile_count]
    by_region_depth = jnp.transpose(frame_depth.reshape(TROWS // 2, 2, TCOLS, BAND, TILE), (0, 2, 1, 3, 4)).reshape(REGIONS, 2, BAND, TILE)
    by_region_color = jnp.transpose(frame_color.reshape(TROWS // 2, 2, TCOLS, BAND, 3, TILE), (0, 2, 1, 3, 4, 5)).reshape(REGIONS, 2, BAND, 3, TILE)
    inverse = jnp.zeros((REGIONS,), jnp.int32).at[owner_map].set(jnp.arange(REGIONS, dtype=jnp.int32))
    region_depth = by_region_depth[inverse]
    region_color = by_region_color[inverse]
    block_means = by_region_color.astype(jnp.float32).reshape(REGIONS, 2, BAND // 8, 8, 3, TILE // 8, 8).mean(axis=(3, 6))
    thumbnail = jnp.transpose(block_means, (0, 3, 1, 2, 4)).reshape(REGIONS, 3, THUMB)
    return region_depth, region_color, thumbnail
```

```python
import functools

import jax
import jax.numpy as jnp
from jax import lax
from jax.experimental import pallas as pl
from jax.experimental.pallas import tpu as pltpu
from jax.sharding import PartitionSpec as P

FAR = 1073741824
HALF = 536870912
MESH = pl.DeviceIdType.MESH


def div_const(value, by):
    if by & (by - 1) == 0:
        return value >> (by.bit_length() - 1)
    return value // by


def merge(first, second):
    key_a, colors_a = first
    key_b, colors_b = second
    nearer = key_b < key_a
    key = jnp.minimum(key_a, key_b)
    return key, [jnp.where(nearer, b, a) for a, b in zip(colors_a, colors_b)]


def load(ref_d, ref_c, index):
    return ref_d[index], [ref_c[index + (c,)] for c in range(3)]


def store(ref_d, ref_c, index, value):
    ref_d[index] = value[0]
    for c in range(3):
        ref_c[index + (c,)] = value[1][c]


def far_pos(z, k, Z):
    if Z == 4:
        flip = Z - 1 - k
        hi, lo = z // 2, z % 2
        hi = 1 - hi if flip >= 2 else hi
        lo = 1 - lo if flip % 2 else lo
        return hi * 2 + lo
    return lax.rem(z + 1 + k, Z)


def kernel(
    dims, own_hbm, slots_hbm, depth_hbm, color_hbm,
    out_d, out_c, out_t,
    own_ref, slots_ref, tab_ref, depth_ref, color_ref,
    cs_d, cs_c, cr_d, cr_c, ys_d, ys_c, yr_d, yr_c, zs_d, zs_c, zr_d, zr_c,
    gath,
    l_sem, c_ss, c_rs, y_ss, y_rs, z_ss, z_rs, g_ss, g_rs, tok_lo, tok_hi,
):
    GX, GY, X, Y, Z = dims
    regions = GX * GY
    slots = slots_ref.shape[1]
    gx = lax.axis_index("gx")
    gy = lax.axis_index("gy")
    core = lax.rem(gx, 2)
    x = lax.div(gx, 2)
    y = lax.rem(gy, Y)
    z = lax.div(gy, Y)
    rank = gx * GY + gy
    tile_cols = GY

    def at(cc, xx, yy, zz):
        return (xx * 2 + cc, zz * Y + yy)

    barrier = pltpu.get_barrier_semaphore()

    def greet(device):
        pl.semaphore_signal(barrier, inc=1, device_id=device, device_id_type=MESH)

    greet(at(1 - core, x, y, z))
    for j in range(1, Y):
        greet(at(core, x, lax.rem(y + j, Y), z))
    for j in range(1, X):
        greet(at(core, lax.rem(x + j, X), y, z))
    has_lo = z > 0
    has_hi = z < Z - 1

    @pl.when(has_lo)
    def _():
        greet(at(core, x, y, z - 1))

    @pl.when(has_hi)
    def _():
        greet(at(core, x, y, z + 1))

    def local(src, dst, k):
        copy = pltpu.make_async_copy(src, dst, l_sem.at[k])
        copy.start()
        return copy

    loads = [
        local(own_hbm, own_ref, 0),
        local(slots_hbm, slots_ref, 1),
        local(depth_hbm, depth_ref.at[pl.ds(0, slots)], 2),
        local(color_hbm, color_ref.at[pl.ds(0, slots)], 3),
    ]

    def token(which):
        @pl.when(has_lo)
        def _():
            pl.semaphore_signal(tok_hi, inc=1, device_id=at(core, x, y, z - 1), device_id_type=MESH)

        @pl.when(has_hi)
        def _():
            pl.semaphore_signal(tok_lo, inc=1, device_id=at(core, x, y, z + 1), device_id_type=MESH)

    def take_token():
        @pl.when(has_lo)
        def _():
            pl.semaphore_wait(tok_lo, 1)

        @pl.when(has_hi)
        def _():
            pl.semaphore_wait(tok_hi, 1)

    depth_ref[slots] = jnp.full(depth_ref.shape[1:], FAR, jnp.int32)
    for c in range(3):
        color_ref[slots, c] = jnp.zeros(color_ref.shape[2:], jnp.bfloat16)

    loads[0].wait()
    loads[1].wait()
    words = (regions + 31) // 32
    bits = (regions - 1).bit_length()
    masks = [[None] * bits for _ in range(words)]
    for r in range(regions):
        owner = own_ref[r]
        for w in range(words):
            one = jnp.int32(1) << (owner & 31)
            if words > 1:
                one = jnp.where((owner >> 5) == w, one, 0)
            for b in range(bits):
                if (r >> b) & 1:
                    masks[w][b] = one if masks[w][b] is None else masks[w][b] | one
    vals = [slots_ref[0, s] for s in range(slots)]
    first = vals[0]
    while len(vals) > 1:
        vals = [jnp.maximum(vals[i], vals[i + 1]) for i in range(0, len(vals) - 1, 2)] + (
            [vals[-1]] if len(vals) % 2 else []
        )
    last = vals[0]
    top = div_const(first, tile_cols)
    left = first - top * tile_cols
    bottom = div_const(last, tile_cols)
    right = last - bottom * tile_cols
    width = right - left + 1
    for p in range(regions):
        region = None
        for b in range(bits):
            bit = ((masks[p // 32][b] >> (p % 32)) & 1) << b
            region = bit if region is None else region | bit
        pair = div_const(region, tile_cols)
        col = region - pair * tile_cols
        in_col = (col >= left) & (col <= right)
        for h in range(2):
            row = pair * 2 + h
            live = (row >= top) & (row <= bottom) & in_col
            tab_ref[p * 2 + h] = jnp.where(live, (row - top) * width + (col - left), slots)

    def own_tile(cc, xx, yy, zz, h):
        slot = tab_ref[((xx * 2 + cc) * GY + zz * Y + yy) * 2 + h]
        return (depth_ref[slot] - HALF) * 2 + core, [color_ref[slot, c] for c in range(3)]

    pending = []

    def remote(src, dst, ss, rs, device):
        return pltpu.make_async_remote_copy(
            src_ref=src, dst_ref=dst, send_sem=ss, recv_sem=rs, device_id=device, device_id_type=MESH
        )

    def send(pairs, sems, device):
        for k, (src, dst) in enumerate(pairs):
            copy = remote(src, dst, sems[0].at[sems[1] + (k,)], sems[2].at[sems[3] + (k,)], device)
            copy.start()
            pending.append(copy)

    def arrived(refs, rs, index):
        for k, ref in enumerate(refs):
            remote(ref, ref, c_ss.at[0, 0, k], rs.at[index + (k,)], (gx, gy)).wait_recv()

    targets_y = [lax.rem(y + 1 + i, Y) for i in range(Y)]
    targets_z = [far_pos(z, k, Z) for k in range(Z)]
    targets_x = [lax.rem(x + 1 + j, X) for j in range(X)]

    loads[2].wait()
    loads[3].wait()

    for i in range(Y):
        for k in range(Z):
            for j in range(X):
                for h in range(2):
                    store(cs_d, cs_c, (i, k, j, h), own_tile(1 - core, targets_x[j], targets_y[i], targets_z[k], h))
            if i == 0 and k == 0:
                near = X + Y - 1 + jnp.where(has_lo, 1, 0) + jnp.where(has_hi, 1, 0)
                pl.semaphore_wait(barrier, near)
            send(
                [(cs_d.at[i, k], cr_d.at[i, k]), (cs_c.at[i, k], cr_c.at[i, k])],
                (c_ss, (i, k), c_rs, (i, k)),
                at(1 - core, x, y, z),
            )
        if i == 0:
            token(0)

    for i in range(Y):
        mine = i == Y - 1
        for k in range(Z):
            arrived([cr_d.at[i, k], cr_c.at[i, k]], c_rs, (i, k))
            for j in range(X):
                for h in range(2):
                    value = merge(
                        own_tile(core, targets_x[j], targets_y[i], targets_z[k], h),
                        load(cr_d, cr_c, (i, k, j, h)),
                    )
                    if mine:
                        store(yr_d, yr_c, (k, j, y, h), value)
                    else:
                        store(ys_d, ys_c, (i, k, j, h), value)
                if not mine:
                    send(
                        [(ys_d.at[i, k, j], yr_d.at[k, j, y]), (ys_c.at[i, k, j], yr_c.at[k, j, y])],
                        (y_ss, (i, k, j), y_rs, (k, j, y)),
                        at(core, x, targets_y[i], z),
                    )
        if i == 0:
            take_token()
            token(1)

    take_token()
    token(2)
    take_token()

    for k in range(Z):
        for j in range(X):
            for i in range(Y - 1):
                yy = targets_y[i]
                arrived([yr_d.at[k, j, yy], yr_c.at[k, j, yy]], y_rs, (k, j, yy))
            mine = k == Z - 1 and j == X - 1
            for h in range(2):
                value = load(yr_d, yr_c, (k, j, 0, h))
                for q in range(1, Y):
                    value = merge(value, load(yr_d, yr_c, (k, j, q, h)))
                if mine:
                    store(zr_d, zr_c, (x, z, h), value)
                else:
                    store(zs_d, zs_c, (k, j, h), value)
            if not mine:
                send(
                    [(zs_d.at[k, j], zr_d.at[x, z]), (zs_c.at[k, j], zr_c.at[x, z])],
                    (z_ss, (k, j), z_rs, (x, z)),
                    at(core, targets_x[j], y, targets_z[k]),
                )

    lane_k = lax.broadcasted_iota(jnp.int32, (128, 128), 0) // 8
    lane_l = lax.broadcasted_iota(jnp.int32, (128, 128), 1)
    groups = []
    for h in range(2):
        hit = (lane_l == lane_k + 32 * h) | (lane_l == lane_k + 32 * h + 80)
        groups.append(jnp.where(hit, 1.0 / 64.0, 0.0).astype(jnp.bfloat16))

    for k in range(Z):
        for j in range(X):
            if k == Z - 1 and j == X - 1:
                continue
            xx, zz = targets_x[j], targets_z[k]
            arrived([zr_d.at[xx, zz], zr_c.at[xx, zz]], z_rs, (xx, zz))

    sums = [None] * 3
    row = lax.broadcasted_iota(jnp.int32, (16, 128), 0)
    lane = lax.broadcasted_iota(jnp.int32, (16, 128), 1)
    keep = (row < 8) == (lane < 64)
    for h in range(2):
        value = None
        for xx in range(X):
            part = load(zr_d, zr_c, (xx, 0, h))
            for zz in range(1, Z):
                part = merge(part, load(zr_d, zr_c, (xx, zz, h)))
            part = (part[0] >> 1, part[1])
            value = part if value is None else merge(value, part)
        out_d[h] = value[0] + HALF
        for c in range(3):
            color = value[1][c]
            out_c[h, c] = color
            part = jnp.dot(color, groups[h], preferred_element_type=jnp.float32)
            part = jnp.where(keep, part, 0.0)
            sums[c] = part if sums[c] is None else sums[c] + part
    rows = []
    for c in range(3):
        total = jnp.sum(sums[c], axis=0, keepdims=True)
        rows.append(total + pltpu.roll(total, 64, 1))
    lane_row = lax.broadcasted_iota(jnp.int32, (1, 128), 1)
    gath[gx, gy, 0:1, :] = jnp.where(lane_row < 64, rows[0], rows[1])
    gath[gx, gy, 1:2, :] = rows[2]

    others = []
    for k in range(Z):
        for j in range(X):
            for i in range(Y):
                for cc in (1 - core, core):
                    others.append(at(cc, targets_x[j], targets_y[i], targets_z[k]))
    others.pop()
    for n, device in enumerate(others):
        copy = remote(gath.at[gx, gy], gath.at[gx, gy], g_ss.at[n], g_rs.at[gx, gy], device)
        copy.start()
        pending.append(copy)
    for n, (ox, oy) in enumerate(others):
        remote(gath.at[ox, oy], gath.at[ox, oy], g_ss.at[n], g_rs.at[ox, oy], (gx, gy)).wait_recv()
    for r in range(regions):
        owner = own_ref[r]
        owner_x = div_const(owner, GY)
        out_t[r] = gath[owner_x, owner - owner_x * GY]
    for copy in pending:
        copy.wait_send()


def finish(in_d, in_c, in_t, out_d, out_c, out_t):
    out_d[...] = in_d[...]
    out_c[...] = in_c[...]
    side = out_t.shape[2]
    upper = in_t[:, 0, :]
    out_t[0] = upper[:, :side]
    out_t[1] = upper[:, side:]
    out_t[2] = in_t[:, 1, :][:, :side]


def shards(slot_tiles, owner_map, slot_depth, slot_color):
    GX = lax.axis_size("gx")
    GY = lax.axis_size("gy")
    X, Z = GX // 2, 4
    Y = GY // Z
    regions = GX * GY
    slots, band, width = slot_depth.shape[1:]
    depth = slot_depth[0]
    color = jnp.transpose(slot_color[0], (0, 2, 1, 3))

    def pair(*lead):
        return [
            pltpu.VMEM(lead + (band, width), jnp.int32),
            pltpu.VMEM(lead + (3, band, width), jnp.bfloat16),
        ]

    dma = lambda *shape: pltpu.SemaphoreType.DMA(shape)
    vmem = pl.BlockSpec(memory_space=pltpu.VMEM)
    hbm = pl.BlockSpec(memory_space=pl.ANY)
    out_d, out_c, out_t = pl.pallas_call(
        functools.partial(kernel, (GX, GY, X, Y, Z)),
        out_shape=(
            pltpu.VMEM((2, band, width), jnp.int32),
            pltpu.VMEM((2, 3, band, width), jnp.bfloat16),
            pltpu.VMEM((regions, 2, width), jnp.float32),
        ),
        in_specs=[hbm, hbm, hbm, hbm],
        out_specs=(vmem, vmem, vmem),
        scratch_shapes=[
            pltpu.SMEM((regions,), jnp.int32),
            pltpu.SMEM((1, slots), jnp.int32),
            pltpu.SMEM((2 * regions,), jnp.int32),
            *pair(slots + 1),
            *pair(Y, Z, X, 2), *pair(Y, Z, X, 2),
            *pair(Y, Z, X, 2), *pair(Z, X, Y, 2),
            *pair(Z, X, 2), *pair(X, Z, 2),
            pltpu.VMEM((GX, GY, 2, width), jnp.float32),
            dma(4),
            dma(Y, Z, 2), dma(Y, Z, 2),
            dma(Y, Z, X, 2), dma(Z, X, Y, 2),
            dma(Z, X, 2), dma(X, Z, 2),
            dma(regions), dma(GX, GY),
            pltpu.SemaphoreType.REGULAR, pltpu.SemaphoreType.REGULAR,
        ],
        compiler_params=pltpu.CompilerParams(collective_id=0, has_side_effects=True),
    )(owner_map, slot_tiles, depth, color)
    out_d, out_c, out_t = pl.pallas_call(
        finish,
        out_shape=(
            jax.ShapeDtypeStruct((2, band, width), jnp.int32),
            jax.ShapeDtypeStruct((2, 3, band, width), jnp.bfloat16),
            jax.ShapeDtypeStruct((3, regions, width // 2), jnp.float32),
        ),
        in_specs=[vmem, vmem, vmem],
        out_specs=(vmem, vmem, vmem),
    )(*(pltpu.with_memory_space_constraint(a, pltpu.VMEM) for a in (out_d, out_c, out_t)))
    thumbnail = jnp.transpose(out_t, (1, 0, 2))
    return (out_d[None], jnp.transpose(out_c, (0, 2, 1, 3))[None], thumbnail)


def solution(mesh):
    placed = (
        P(("gx", "gy"), None),
        P(),
        P(("gx", "gy"), None, None, None),
        P(("gx", "gy"), None, None, None, None),
    )
    return jax.shard_map(
        shards,
        mesh=mesh,
        in_specs=placed,
        out_specs=(P(("gx", "gy"), None, None, None), P(("gx", "gy"), None, None, None, None), P()),
        check_vma=False,
    )
```

```python
import functools

import jax
import jax.numpy as jnp
from jax import lax
from jax.experimental import pallas as pl
from jax.experimental.pallas import tpu as pltpu
from jax.sharding import PartitionSpec as P

FAR = 1073741824
HALF = 536870912
MESH = pl.DeviceIdType.MESH


def div_const(value, by):
    if by & (by - 1) == 0:
        return value >> (by.bit_length() - 1)
    return value // by


def merge(first, second):
    key_a, colors_a = first
    key_b, colors_b = second
    nearer = key_b < key_a
    key = jnp.minimum(key_a, key_b)
    return key, [jnp.where(nearer, b, a) for a, b in zip(colors_a, colors_b)]


def load(ref_d, ref_c, index):
    return ref_d[index], [ref_c[index + (c,)] for c in range(3)]


def store(ref_d, ref_c, index, value):
    ref_d[index] = value[0]
    for c in range(3):
        ref_c[index + (c,)] = value[1][c]


def far_pos(z, k, Z):
    if Z == 4:
        flip = Z - 1 - k
        hi, lo = z // 2, z % 2
        hi = 1 - hi if flip >= 2 else hi
        lo = 1 - lo if flip % 2 else lo
        return hi * 2 + lo
    return lax.rem(z + 1 + k, Z)


def kernel(
    dims, own_hbm, slots_hbm, depth_hbm, color_hbm,
    out_d, out_c, out_t,
    own_ref, slots_ref, tab_ref, depth_ref, color_ref,
    cs_d, cs_c, cr_d, cr_c, ys_d, ys_c, yr_d, yr_c, zs_d, zs_c, zr_d, zr_c,
    gath,
    l_sem, s_sem, c_rs, y_rs, z_rs, g_rs, tok_lo, tok_hi,
):
    GX, GY, X, Y, Z = dims
    regions = GX * GY
    slots = slots_ref.shape[1]
    gx = lax.axis_index("gx")
    gy = lax.axis_index("gy")
    core = lax.rem(gx, 2)
    x = lax.div(gx, 2)
    y = lax.rem(gy, Y)
    z = lax.div(gy, Y)
    rank = gx * GY + gy
    tile_cols = GY

    def at(cc, xx, yy, zz):
        return (xx * 2 + cc, zz * Y + yy)

    barrier = pltpu.get_barrier_semaphore()

    def greet(device):
        pl.semaphore_signal(barrier, inc=1, device_id=device, device_id_type=MESH)

    greet(at(1 - core, x, y, z))
    for j in range(1, Y):
        greet(at(core, x, lax.rem(y + j, Y), z))
    for j in range(1, X):
        greet(at(core, lax.rem(x + j, X), y, z))
    has_lo = z > 0
    has_hi = z < Z - 1

    @pl.when(has_lo)
    def _():
        greet(at(core, x, y, z - 1))

    @pl.when(has_hi)
    def _():
        greet(at(core, x, y, z + 1))

    def local(src, dst, k):
        copy = pltpu.make_async_copy(src, dst, l_sem.at[k])
        copy.start()
        return copy

    loads = [
        local(own_hbm, own_ref, 0),
        local(slots_hbm, slots_ref, 1),
        local(depth_hbm, depth_ref.at[pl.ds(0, slots)], 2),
        local(color_hbm, color_ref.at[pl.ds(0, slots)], 3),
    ]

    def token(which):
        @pl.when(has_lo)
        def _():
            pl.semaphore_signal(tok_hi, inc=1, device_id=at(core, x, y, z - 1), device_id_type=MESH)

        @pl.when(has_hi)
        def _():
            pl.semaphore_signal(tok_lo, inc=1, device_id=at(core, x, y, z + 1), device_id_type=MESH)

    def take_token():
        @pl.when(has_lo)
        def _():
            pl.semaphore_wait(tok_lo, 1)

        @pl.when(has_hi)
        def _():
            pl.semaphore_wait(tok_hi, 1)

    depth_ref[slots] = jnp.full(depth_ref.shape[1:], FAR, jnp.int32)
    for c in range(3):
        color_ref[slots, c] = jnp.zeros(color_ref.shape[2:], jnp.bfloat16)

    loads[0].wait()
    loads[1].wait()
    words = (regions + 31) // 32
    bits = (regions - 1).bit_length()
    masks = [[None] * bits for _ in range(words)]
    for r in range(regions):
        owner = own_ref[r]
        for w in range(words):
            one = jnp.int32(1) << (owner & 31)
            if words > 1:
                one = jnp.where((owner >> 5) == w, one, 0)
            for b in range(bits):
                if (r >> b) & 1:
                    masks[w][b] = one if masks[w][b] is None else masks[w][b] | one
    vals = [slots_ref[0, s] for s in range(slots)]
    first = vals[0]
    while len(vals) > 1:
        vals = [jnp.maximum(vals[i], vals[i + 1]) for i in range(0, len(vals) - 1, 2)] + (
            [vals[-1]] if len(vals) % 2 else []
        )
    last = vals[0]
    top = div_const(first, tile_cols)
    left = first - top * tile_cols
    bottom = div_const(last, tile_cols)
    right = last - bottom * tile_cols
    width = right - left + 1
    for p in range(regions):
        region = None
        for b in range(bits):
            bit = ((masks[p // 32][b] >> (p % 32)) & 1) << b
            region = bit if region is None else region | bit
        pair = div_const(region, tile_cols)
        col = region - pair * tile_cols
        in_col = (col >= left) & (col <= right)
        for h in range(2):
            row = pair * 2 + h
            live = (row >= top) & (row <= bottom) & in_col
            tab_ref[p * 2 + h] = jnp.where(live, (row - top) * width + (col - left), slots)

    def own_tile(cc, xx, yy, zz, h):
        slot = tab_ref[((xx * 2 + cc) * GY + zz * Y + yy) * 2 + h]
        return (depth_ref[slot] - HALF) * 2 + core, [color_ref[slot, c] for c in range(3)]

    def remote(src, dst, ss, rs, device):
        return pltpu.make_async_remote_copy(
            src_ref=src, dst_ref=dst, send_sem=ss, recv_sem=rs, device_id=device, device_id_type=MESH
        )

    def send(pairs, which, rs, device):
        for k, (src, dst) in enumerate(pairs):
            remote(src, dst, s_sem.at[which + k], rs, device).start()

    def take(ref, rs):
        remote(ref, ref, s_sem.at[0], rs, (gx, gy)).wait_recv()

    def arrived(units, rs):
        take(depth_ref.at[pl.ds(0, 5 * units)], rs)

    def drained(ref, which):
        remote(ref, ref, s_sem.at[which], g_rs, (gx, gy)).wait_send()

    targets_y = [lax.rem(y + 1 + i, Y) for i in range(Y)]
    targets_z = [far_pos(z, k, Z) for k in range(Z)]
    targets_x = [lax.rem(x + 1 + j, X) for j in range(X)]

    loads[2].wait()
    loads[3].wait()

    for i in range(Y):
        for k in range(Z):
            for j in range(X):
                for h in range(2):
                    store(cs_d, cs_c, (i, k, j, h), own_tile(1 - core, targets_x[j], targets_y[i], targets_z[k], h))
            if i == 0 and k == 0:
                near = X + Y - 1 + jnp.where(has_lo, 1, 0) + jnp.where(has_hi, 1, 0)
                pl.semaphore_wait(barrier, near)
            send(
                [(cs_d.at[i, k], cr_d.at[i, k]), (cs_c.at[i, k], cr_c.at[i, k])],
                0, c_rs.at[i, k],
                at(1 - core, x, y, z),
            )
        if i == 0:
            token(0)

    for i in range(Y):
        mine = i == Y - 1
        for k in range(Z):
            arrived(X, c_rs.at[i, k])
            for j in range(X):
                for h in range(2):
                    value = merge(
                        own_tile(core, targets_x[j], targets_y[i], targets_z[k], h),
                        load(cr_d, cr_c, (i, k, j, h)),
                    )
                    if mine:
                        store(yr_d, yr_c, (k, j, y, h), value)
                    else:
                        store(ys_d, ys_c, (i, k, j, h), value)
                if not mine:
                    send(
                        [(ys_d.at[i, k, j], yr_d.at[k, j, y]), (ys_c.at[i, k, j], yr_c.at[k, j, y])],
                        2, y_rs.at[i, k, j],
                        at(core, x, targets_y[i], z),
                    )
        if i == 0:
            take_token()
            token(1)

    take_token()
    token(2)
    take_token()

    for k in range(Z):
        for j in range(X):
            for i in range(Y - 1):
                arrived(1, y_rs.at[i, k, j])
            mine = k == Z - 1 and j == X - 1
            for h in range(2):
                value = load(yr_d, yr_c, (k, j, 0, h))
                for q in range(1, Y):
                    value = merge(value, load(yr_d, yr_c, (k, j, q, h)))
                if mine:
                    store(zr_d, zr_c, (x, z, h), value)
                else:
                    store(zs_d, zs_c, (k * X + j, h), value)
            if not mine:
                send(
                    [(zs_d.at[k * X + j], zr_d.at[x, z]), (zs_c.at[k * X + j], zr_c.at[x, z])],
                    4, z_rs.at[x, z],
                    at(core, targets_x[j], y, targets_z[k]),
                )

    lane_k = lax.broadcasted_iota(jnp.int32, (128, 128), 0) // 8
    lane_l = lax.broadcasted_iota(jnp.int32, (128, 128), 1)
    groups = []
    for h in range(2):
        hit = (lane_l == lane_k + 32 * h) | (lane_l == lane_k + 32 * h + 80)
        groups.append(jnp.where(hit, 1.0 / 64.0, 0.0).astype(jnp.bfloat16))

    for k in range(Z):
        for j in range(X):
            if k == Z - 1 and j == X - 1:
                continue
            xx, zz = targets_x[j], targets_z[k]
            arrived(1, z_rs.at[xx, zz])

    sums = [None] * 3
    row = lax.broadcasted_iota(jnp.int32, (16, 128), 0)
    lane = lax.broadcasted_iota(jnp.int32, (16, 128), 1)
    keep = (row < 8) == (lane < 64)
    for h in range(2):
        value = None
        for xx in range(X):
            part = load(zr_d, zr_c, (xx, 0, h))
            for zz in range(1, Z):
                part = merge(part, load(zr_d, zr_c, (xx, zz, h)))
            part = (part[0] >> 1, part[1])
            value = part if value is None else merge(value, part)
        out_d[h] = value[0] + HALF
        for c in range(3):
            color = value[1][c]
            out_c[h, c] = color
            part = jnp.dot(color, groups[h], preferred_element_type=jnp.float32)
            part = jnp.where(keep, part, 0.0)
            sums[c] = part if sums[c] is None else sums[c] + part
    rows = []
    for c in range(3):
        total = jnp.sum(sums[c], axis=0, keepdims=True)
        rows.append(total + pltpu.roll(total, 64, 1))
    lane_row = lax.broadcasted_iota(jnp.int32, (1, 128), 1)
    gath[rank, 0:1, :] = jnp.where(lane_row < 64, rows[0], rows[1])
    gath[rank, 1:2, :] = rows[2]

    others = []
    for k in range(Z):
        for j in range(X):
            for i in range(Y):
                for cc in (1 - core, core):
                    others.append(at(cc, targets_x[j], targets_y[i], targets_z[k]))
    others.pop()
    for device in others:
        remote(gath.at[rank], gath.at[rank], s_sem.at[6], g_rs, device).start()
    take(gath.at[pl.ds(0, regions - 1)], g_rs)
    for r in range(regions):
        out_t[r] = gath[own_ref[r]]
    drained(cs_d, 0)
    drained(cs_c, 1)
    drained(ys_d, 2)
    drained(ys_c, 3)
    drained(zs_d, 4)
    drained(zs_c, 5)
    drained(gath.at[pl.ds(0, regions - 1)], 6)


def finish(in_d, in_c, in_t, out_d, out_c, out_t):
    out_d[...] = in_d[...]
    out_c[...] = in_c[...]
    side = out_t.shape[2]
    upper = in_t[:, 0, :]
    out_t[0] = upper[:, :side]
    out_t[1] = upper[:, side:]
    out_t[2] = in_t[:, 1, :][:, :side]


def shards(slot_tiles, owner_map, slot_depth, slot_color):
    GX = lax.axis_size("gx")
    GY = lax.axis_size("gy")
    X, Z = GX // 2, 4
    Y = GY // Z
    regions = GX * GY
    slots, band, width = slot_depth.shape[1:]
    depth = slot_depth[0]
    color = jnp.transpose(slot_color[0], (0, 2, 1, 3))

    def pair(*lead):
        return [
            pltpu.VMEM(lead + (band, width), jnp.int32),
            pltpu.VMEM(lead + (3, band, width), jnp.bfloat16),
        ]

    dma = lambda *shape: pltpu.SemaphoreType.DMA(shape)
    vmem = pl.BlockSpec(memory_space=pltpu.VMEM)
    hbm = pl.BlockSpec(memory_space=pl.ANY)
    out_d, out_c, out_t = pl.pallas_call(
        functools.partial(kernel, (GX, GY, X, Y, Z)),
        out_shape=(
            pltpu.VMEM((2, band, width), jnp.int32),
            pltpu.VMEM((2, 3, band, width), jnp.bfloat16),
            pltpu.VMEM((regions, 2, width), jnp.float32),
        ),
        in_specs=[hbm, hbm, hbm, hbm],
        out_specs=(vmem, vmem, vmem),
        scratch_shapes=[
            pltpu.SMEM((regions,), jnp.int32),
            pltpu.SMEM((1, slots), jnp.int32),
            pltpu.SMEM((2 * regions,), jnp.int32),
            *pair(slots + 1),
            *pair(Y, Z, X, 2), *pair(Y, Z, X, 2),
            *pair(Y - 1, Z, X, 2), *pair(Z, X, Y, 2),
            *pair(Z * X - 1, 2), *pair(X, Z, 2),
            pltpu.VMEM((regions, 2, width), jnp.float32),
            dma(4), dma(7),
            dma(Y, Z), dma(Y - 1, Z, X), dma(X, Z), pltpu.SemaphoreType.DMA,
            pltpu.SemaphoreType.REGULAR, pltpu.SemaphoreType.REGULAR,
        ],
        compiler_params=pltpu.CompilerParams(collective_id=0, has_side_effects=True),
    )(owner_map, slot_tiles, depth, color)
    out_d, out_c, out_t = pl.pallas_call(
        finish,
        out_shape=(
            jax.ShapeDtypeStruct((2, band, width), jnp.int32),
            jax.ShapeDtypeStruct((2, 3, band, width), jnp.bfloat16),
            jax.ShapeDtypeStruct((3, regions, width // 2), jnp.float32),
        ),
        in_specs=[vmem, vmem, vmem],
        out_specs=(vmem, vmem, vmem),
    )(*(pltpu.with_memory_space_constraint(a, pltpu.VMEM) for a in (out_d, out_c, out_t)))
    thumbnail = jnp.transpose(out_t, (1, 0, 2))
    return (out_d[None], jnp.transpose(out_c, (0, 2, 1, 3))[None], thumbnail)


def solution(mesh):
    placed = (
        P(("gx", "gy"), None),
        P(),
        P(("gx", "gy"), None, None, None),
        P(("gx", "gy"), None, None, None, None),
    )
    return jax.shard_map(
        shards,
        mesh=mesh,
        in_specs=placed,
        out_specs=(P(("gx", "gy"), None, None, None), P(("gx", "gy"), None, None, None, None), P()),
        check_vma=False,
    )
```

```python
import functools

import jax
import jax.numpy as jnp
from jax import lax
from jax.experimental import pallas as pl
from jax.experimental.pallas import tpu as pltpu
from jax.sharding import PartitionSpec as P

FAR = 1073741824
HALF = 536870912
LOWEST = -2147483648
LARGEST = 2147483647
MESH = pl.DeviceIdType.MESH


def div_const(value, by):
    if by & (by - 1) == 0:
        return value >> (by.bit_length() - 1)
    return value // by


def merge(first, second):
    key_a, colors_a = first
    key_b, colors_b = second
    nearer = key_b < key_a
    key = jnp.minimum(key_a, key_b)
    return key, [jnp.where(nearer, b, a) for a, b in zip(colors_a, colors_b)]


def merge_tagged(first, second):
    key, colors = merge(first, second)
    unnamed = first[1][0] < 0
    return key, [jnp.where(unnamed, b, c) for b, c in zip(second[1], colors)]


def fold(values, how):
    total = values[0]
    for value in values[1:]:
        total = how(total, value)
    return total


def load(ref_d, ref_c, index):
    return ref_d[index], [ref_c[index + (c,)] for c in range(3)]


def store(ref_d, ref_c, index, value):
    ref_d[index] = value[0]
    for c in range(3):
        ref_c[index + (c,)] = value[1][c]


def far_pos(z, k, Z):
    if Z == 4:
        flip = Z - 1 - k
        hi, lo = z // 2, z % 2
        hi = 1 - hi if flip >= 2 else hi
        lo = 1 - lo if flip % 2 else lo
        return hi * 2 + lo
    return lax.rem(z + 1 + k, Z)


def plan(X, Y, Z):
    halves_a, halves_b = ((0,), (1,)) if X == 2 else ((0, 1), ())
    first, second = [], []
    for near in (False, True):
        for k in range(Z):
            for i in range(Y - 1):
                for j in [X - 1] if near else range(X - 1):
                    first += [("a", h, j, i, k) for h in halves_a]
            for j in range(X - 1):
                for i in [Y - 1] if near else range(Y - 1):
                    first += [("b", h, j, i, k) for h in halves_b]
    for k in range(Z):
        second += [("a", h, j, Y - 1, k) for j in range(X) for h in halves_a]
        second += [("b", h, X - 1, i, k) for i in range(Y) for h in halves_b]
    return halves_a, halves_b, first, second


def sent_tiles(X, Y, Z):
    halves_a, halves_b, first, second = plan(X, Y, Z)
    na, nb = len(halves_a), len(halves_b)
    rest = na * (X * (Z - 1) + X - 1) + nb * (Z * (Y - 1) + Z - 1)
    return len(first) * 2 + len(second) + rest


def kernel(
    dims, own_hbm, slots_hbm, depth_hbm, color_hbm,
    out_d, out_c, out_t,
    own_ref, slots_ref, tab_ref, depth_ref, color_ref,
    s_d, s_c, cr_d, cr_c, ay_d, ay_c, az_d, az_c, ax_d, ax_c, bx_d, bx_c, by_d, by_c, bz_d, bz_c,
    gath,
    l_sem, s_sem, c_rs, ay_rs, az_rs, ax_rs, bx_rs, by_rs, bz_rs, g_rs, tok_lo, tok_hi,
):
    GX, GY, X, Y, Z = dims
    regions = GX * GY
    slots = slots_ref.shape[1]
    gx = lax.axis_index("gx")
    gy = lax.axis_index("gy")
    core = lax.rem(gx, 2)
    x = lax.div(gx, 2)
    y = lax.rem(gy, Y)
    z = lax.div(gy, Y)
    rank = gx * GY + gy
    tile_cols = GY

    def at(cc, xx, yy, zz):
        return (xx * 2 + cc, zz * Y + yy)

    barrier = pltpu.get_barrier_semaphore()

    def greet(device):
        pl.semaphore_signal(barrier, inc=1, device_id=device, device_id_type=MESH)

    greet(at(1 - core, x, y, z))
    for j in range(1, Y):
        greet(at(core, x, lax.rem(y + j, Y), z))
    for j in range(1, X):
        greet(at(core, lax.rem(x + j, X), y, z))
    has_lo = z > 0
    has_hi = z < Z - 1

    @pl.when(has_lo)
    def _():
        greet(at(core, x, y, z - 1))

    @pl.when(has_hi)
    def _():
        greet(at(core, x, y, z + 1))

    def local(src, dst, k):
        copy = pltpu.make_async_copy(src, dst, l_sem.at[k])
        copy.start()
        return copy

    loads = [
        local(own_hbm, own_ref, 0),
        local(slots_hbm, slots_ref, 1),
        local(depth_hbm, depth_ref.at[pl.ds(0, slots)], 2),
        local(color_hbm, color_ref.at[pl.ds(0, slots)], 3),
    ]

    def token():
        @pl.when(has_lo)
        def _():
            pl.semaphore_signal(tok_hi, inc=1, device_id=at(core, x, y, z - 1), device_id_type=MESH)

        @pl.when(has_hi)
        def _():
            pl.semaphore_signal(tok_lo, inc=1, device_id=at(core, x, y, z + 1), device_id_type=MESH)

    def take_token():
        @pl.when(has_lo)
        def _():
            pl.semaphore_wait(tok_lo, 1)

        @pl.when(has_hi)
        def _():
            pl.semaphore_wait(tok_hi, 1)

    depth_ref[slots] = jnp.full(depth_ref.shape[1:], FAR, jnp.int32)
    for c in range(3):
        color_ref[slots, c] = jnp.full(color_ref.shape[2:], -1.0, jnp.bfloat16)

    loads[0].wait()
    loads[1].wait()
    words = (regions + 31) // 32
    bits = (regions - 1).bit_length()
    masks = [[None] * bits for _ in range(words)]
    for r in range(regions):
        owner = own_ref[r]
        for w in range(words):
            one = jnp.int32(1) << (owner & 31)
            if words > 1:
                one = jnp.where((owner >> 5) == w, one, 0)
            for b in range(bits):
                if (r >> b) & 1:
                    masks[w][b] = one if masks[w][b] is None else masks[w][b] | one
    vals = [slots_ref[0, s] for s in range(slots)]
    first = vals[0]
    while len(vals) > 1:
        vals = [jnp.maximum(vals[i], vals[i + 1]) for i in range(0, len(vals) - 1, 2)] + (
            [vals[-1]] if len(vals) % 2 else []
        )
    last = vals[0]
    top = div_const(first, tile_cols)
    left = first - top * tile_cols
    bottom = div_const(last, tile_cols)
    right = last - bottom * tile_cols
    width = right - left + 1
    for p in range(regions):
        region = None
        for b in range(bits):
            bit = ((masks[p // 32][b] >> (p % 32)) & 1) << b
            region = bit if region is None else region | bit
        pair = div_const(region, tile_cols)
        col = region - pair * tile_cols
        in_col = (col >= left) & (col <= right)
        for h in range(2):
            row = pair * 2 + h
            live = (row >= top) & (row <= bottom) & in_col
            tab_ref[p * 2 + h] = jnp.where(live, (row - top) * width + (col - left), slots)

    def own_tile(kind, cc, xx, yy, zz, h):
        slot = tab_ref[((xx * 2 + cc) * GY + zz * Y + yy) * 2 + h]
        depth = depth_ref[slot] - HALF
        if kind == "a":
            key = depth * 2 + core
        else:
            key = jnp.maximum(depth * 4 + (x * 2 + core), jnp.where(slot == slots, LARGEST, LOWEST))
        return key, [color_ref[slot, c] for c in range(3)]

    def remote(src, dst, ss, rs, device):
        return pltpu.make_async_remote_copy(
            src_ref=src, dst_ref=dst, send_sem=ss, recv_sem=rs, device_id=device, device_id_type=MESH
        )

    used = [0]

    def post(value):
        n = used[0]
        used[0] += 1
        store(s_d, s_c, (n,), value)
        return n

    def send(n, many, into_d, into_c, at_index, rs, device):
        if many is None:
            src, dst = (n,), (at_index,)
        else:
            src, dst = (pl.ds(n, many),), (pl.ds(at_index, many),)
        remote(s_d.at[src], into_d.at[dst], s_sem.at[0], rs, device).start()
        remote(s_c.at[src], into_c.at[dst], s_sem.at[1], rs, device).start()

    def take(ref, rs):
        remote(ref, ref, s_sem.at[0], rs, (gx, gy)).wait_recv()

    def arrived(tiles, rs):
        if tiles % 2:
            take(depth_ref.at[pl.ds(0, 5 * tiles), pl.ds(0, depth_ref.shape[1] // 2)], rs)
        else:
            take(depth_ref.at[pl.ds(0, 5 * tiles // 2)], rs)

    def drained(ref, which):
        remote(ref, ref, s_sem.at[which], g_rs, (gx, gy)).wait_send()

    ty = [lax.rem(y + 1 + i, Y) for i in range(Y)]
    tz = [far_pos(z, k, Z) for k in range(Z)]
    tx = [lax.rem(x + 1 + j, X) for j in range(X)]
    halves_a, halves_b, first, second = plan(X, Y, Z)
    na, nb = len(halves_a), len(halves_b)
    tiles = first + second
    chunk = len(tiles) // c_rs.shape[0]

    loads[2].wait()
    loads[3].wait()

    for q in range(c_rs.shape[0]):
        for kind, h, j, i, k in tiles[q * chunk : (q + 1) * chunk]:
            n = post(own_tile(kind, 1 - core, tx[j], ty[i], tz[k], h))
        if q == 0:
            near = X + Y - 1 + jnp.where(has_lo, 1, 0) + jnp.where(has_hi, 1, 0)
            pl.semaphore_wait(barrier, near)
        send(q * chunk, chunk, cr_d, cr_c, q * chunk, c_rs.at[q], at(1 - core, x, y, z))
        if q == 0:
            token()

    def ay_at(h, j, k, yy):
        return ((k * X + j) * na + halves_a.index(h)) * Y + yy

    def az_at(h, j, zz):
        return (j * na + halves_a.index(h)) * Z + zz

    def ax_at(h, xx):
        return halves_a.index(h) * X + xx

    def bx_at(h, i, k, xx):
        return ((k * Y + i) * nb + halves_b.index(h)) * X + xx

    def by_at(h, k, yy):
        return (k * nb + halves_b.index(h)) * Y + yy

    def bz_at(h, zz):
        return halves_b.index(h) * Z + zz

    for n, (kind, h, j, i, k) in enumerate(tiles):
        if n % chunk == 0:
            arrived(chunk, c_rs.at[n // chunk])
        how = merge if kind == "a" else merge_tagged
        value = how(own_tile(kind, core, tx[j], ty[i], tz[k], h), load(cr_d, cr_c, (n,)))
        if n >= len(first):
            if kind == "a":
                store(ay_d, ay_c, (ay_at(h, j, k, y),), value)
            else:
                store(bx_d, bx_c, (bx_at(h, i, k, x),), value)
        elif kind == "a":
            send(post(value), None, ay_d, ay_c, ay_at(h, j, k, y), ay_rs.at[i, k, j, halves_a.index(h)], at(core, x, ty[i], z))
        else:
            send(post(value), None, bx_d, bx_c, bx_at(h, i, k, x), bx_rs.at[j, k, i, halves_b.index(h)], at(core, tx[j], y, z))
        if n == len(first) - 1:
            for _ in range(Z - 3):
                take_token()
                token()
    take_token()

    def step_a(j, k):
        for h in halves_a:
            for i in range(Y - 1):
                arrived(1, ay_rs.at[i, k, j, halves_a.index(h)])
            value = fold([load(ay_d, ay_c, (ay_at(h, j, k, q),)) for q in range(Y)], merge)
            if k == Z - 1:
                store(az_d, az_c, (az_at(h, j, z),), value)
            else:
                send(post(value), None, az_d, az_c, az_at(h, j, z), az_rs.at[k, j, halves_a.index(h)], at(core, x, y, tz[k]))

    def step_bx(i, k):
        for h in halves_b:
            for j in range(X - 1):
                arrived(1, bx_rs.at[j, k, i, halves_b.index(h)])
            value = fold([load(bx_d, bx_c, (bx_at(h, i, k, q),)) for q in range(X)], merge_tagged)
            if i == Y - 1:
                store(by_d, by_c, (by_at(h, k, y),), value)
            else:
                send(post(value), None, by_d, by_c, by_at(h, k, y), by_rs.at[i, k, halves_b.index(h)], at(core, x, ty[i], z))

    def step_by(k):
        for h in halves_b:
            for i in range(Y - 1):
                arrived(1, by_rs.at[i, k, halves_b.index(h)])
            value = fold([load(by_d, by_c, (by_at(h, k, q),)) for q in range(Y)], merge_tagged)
            if k == Z - 1:
                store(bz_d, bz_c, (bz_at(h, z),), value)
            else:
                send(post(value), None, bz_d, bz_c, bz_at(h, z), bz_rs.at[k, halves_b.index(h)], at(core, x, y, tz[k]))

    for k in range(Z):
        for i in range(Y - 1):
            step_bx(i, k)
        for j in range(X - 1):
            step_a(j, k)
    for k in range(Z):
        step_a(X - 1, k)
        step_bx(Y - 1, k)
    for k in range(Z):
        step_by(k)

    def step_az(j):
        for h in halves_a:
            for k in range(Z - 1):
                arrived(1, az_rs.at[k, j, halves_a.index(h)])
            key, colors = fold([load(az_d, az_c, (az_at(h, j, q),)) for q in range(Z)], merge)
            value = (key >> 1, colors)
            if j == X - 1:
                store(ax_d, ax_c, (ax_at(h, x),), value)
            else:
                send(post(value), None, ax_d, ax_c, ax_at(h, x), ax_rs.at[j, halves_a.index(h)], at(core, tx[j], y, z))

    for j in range(X):
        step_az(j)

    lane_k = lax.broadcasted_iota(jnp.int32, (128, 128), 0) // 8
    lane_l = lax.broadcasted_iota(jnp.int32, (128, 128), 1)
    groups = []
    for h in range(2):
        hit = (lane_l == lane_k + 32 * h) | (lane_l == lane_k + 32 * h + 80)
        groups.append(jnp.where(hit, 1.0 / 64.0, 0.0).astype(jnp.bfloat16))

    sums = [None] * 3
    row = lax.broadcasted_iota(jnp.int32, (16, 128), 0)
    lane = lax.broadcasted_iota(jnp.int32, (16, 128), 1)
    keep = (row < 8) == (lane < 64)
    for h in halves_b + halves_a:
        if h in halves_b:
            for k in range(Z - 1):
                arrived(1, bz_rs.at[k, halves_b.index(h)])
            key, colors = fold([load(bz_d, bz_c, (bz_at(h, q),)) for q in range(Z)], merge_tagged)
            depth = jnp.where(colors[0].astype(jnp.float32) < 0, FAR, (key >> 2) + HALF)
        else:
            for j in range(X - 1):
                arrived(1, ax_rs.at[j, halves_a.index(h)])
            key, colors = fold([load(ax_d, ax_c, (ax_at(h, q),)) for q in range(X)], merge)
            depth = key + HALF
        out_d[h] = depth
        for c in range(3):
            color = jnp.maximum(colors[c], jnp.zeros((), jnp.bfloat16))
            out_c[h, c] = color
            part = jnp.dot(color, groups[h], preferred_element_type=jnp.float32)
            part = jnp.where(keep, part, 0.0)
            sums[c] = part if sums[c] is None else sums[c] + part
    rows = []
    for c in range(3):
        total = jnp.sum(sums[c], axis=0, keepdims=True)
        rows.append(total + pltpu.roll(total, 64, 1))
    lane_row = lax.broadcasted_iota(jnp.int32, (1, 128), 1)
    gath[rank, 0:1, :] = jnp.where(lane_row < 64, rows[0], rows[1])
    gath[rank, 1:2, :] = rows[2]

    others = []
    for k in range(Z):
        for j in range(X):
            for i in range(Y):
                for cc in (1 - core, core):
                    others.append(at(cc, tx[j], ty[i], tz[k]))
    others.pop()
    for device in others:
        remote(gath.at[rank], gath.at[rank], s_sem.at[2], g_rs, device).start()
    take(gath.at[pl.ds(0, regions - 1)], g_rs)
    for r in range(regions):
        out_t[r] = gath[own_ref[r]]
    drained(s_d, 0)
    drained(s_c, 1)
    drained(gath.at[pl.ds(0, regions - 1)], 2)


def finish(in_d, in_c, in_t, out_d, out_c, out_t):
    out_d[...] = in_d[...]
    out_c[...] = in_c[...]
    side = out_t.shape[2]
    upper = in_t[:, 0, :]
    out_t[0] = upper[:, :side]
    out_t[1] = upper[:, side:]
    out_t[2] = in_t[:, 1, :][:, :side]


def shards(slot_tiles, owner_map, slot_depth, slot_color):
    GX = lax.axis_size("gx")
    GY = lax.axis_size("gy")
    X, Z = GX // 2, 4
    Y = GY // Z
    regions = GX * GY
    na, nb = (len(halves) for halves in plan(X, Y, Z)[:2])
    slots, band, width = slot_depth.shape[1:]
    depth = slot_depth[0]
    color = jnp.transpose(slot_color[0], (0, 2, 1, 3))

    def pair(*lead):
        return [
            pltpu.VMEM(lead + (band, width), jnp.int32),
            pltpu.VMEM(lead + (3, band, width), jnp.bfloat16),
        ]

    dma = lambda *shape: pltpu.SemaphoreType.DMA(shape)
    vmem = pl.BlockSpec(memory_space=pltpu.VMEM)
    hbm = pl.BlockSpec(memory_space=pl.ANY)
    out_d, out_c, out_t = pl.pallas_call(
        functools.partial(kernel, (GX, GY, X, Y, Z)),
        out_shape=(
            pltpu.VMEM((2, band, width), jnp.int32),
            pltpu.VMEM((2, 3, band, width), jnp.bfloat16),
            pltpu.VMEM((regions, 2, width), jnp.float32),
        ),
        in_specs=[hbm, hbm, hbm, hbm],
        out_specs=(vmem, vmem, vmem),
        scratch_shapes=[
            pltpu.SMEM((regions,), jnp.int32),
            pltpu.SMEM((1, slots), jnp.int32),
            pltpu.SMEM((2 * regions,), jnp.int32),
            *pair(slots + 1),
            *pair(sent_tiles(X, Y, Z)), *pair(regions),
            *pair(na * X * Z * Y), *pair(na * X * Z), *pair(na * X),
            *pair(max(nb * X * Z * Y, 1)), *pair(max(nb * Z * Y, 1)), *pair(max(nb * Z, 1)),
            pltpu.VMEM((regions, 2, width), jnp.float32),
            dma(4), dma(3), dma(8),
            dma(Y - 1, Z, X, na), dma(Z - 1, X, na), dma(X - 1, na),
            dma(X - 1, Z, Y, max(nb, 1)), dma(Y - 1, Z, max(nb, 1)), dma(Z - 1, max(nb, 1)),
            pltpu.SemaphoreType.DMA,
            pltpu.SemaphoreType.REGULAR, pltpu.SemaphoreType.REGULAR,
        ],
        compiler_params=pltpu.CompilerParams(collective_id=0, has_side_effects=True),
    )(owner_map, slot_tiles, depth, color)
    out_d, out_c, out_t = pl.pallas_call(
        finish,
        out_shape=(
            jax.ShapeDtypeStruct((2, band, width), jnp.int32),
            jax.ShapeDtypeStruct((2, 3, band, width), jnp.bfloat16),
            jax.ShapeDtypeStruct((3, regions, width // 2), jnp.float32),
        ),
        in_specs=[vmem, vmem, vmem],
        out_specs=(vmem, vmem, vmem),
    )(*(pltpu.with_memory_space_constraint(a, pltpu.VMEM) for a in (out_d, out_c, out_t)))
    thumbnail = jnp.transpose(out_t, (1, 0, 2))
    return (out_d[None], jnp.transpose(out_c, (0, 2, 1, 3))[None], thumbnail)


def solution(mesh):
    placed = (
        P(("gx", "gy"), None),
        P(),
        P(("gx", "gy"), None, None, None),
        P(("gx", "gy"), None, None, None, None),
    )
    return jax.shard_map(
        shards,
        mesh=mesh,
        in_specs=placed,
        out_specs=(P(("gx", "gy"), None, None, None), P(("gx", "gy"), None, None, None, None), P()),
        check_vma=False,
    )
```
